32 devices in a mesh: rows: 8 (over z, y), protos: 4 (over x, core).
Axes of the slice: x: 2, y: 2, z: 4, core: 2. Of those that a mesh axis runs over, the one named last changes fastest.
Arguments:
- features: bfloat16 [3072, 256], P('rows', 'protos'), may hold values from -12 to 12
- prototypes: bfloat16 [65536, 256], P('protos', 'rows'), may hold values from -8 to 8
- masked_index: int32 [1536], P('rows'), may hold values from 0 to 383
Outputs:
- targets: bfloat16 [1536, 65536], P('rows', 'protos')
The draws below stay inside these ranges and needn't reach their ends.
Inputs may be any that keep to these rules, and one draw needn't show every extreme that they name: Row r of the whole takes patch (r // 192) * 384 + masked_index[r] of features.
All inputs are finite; a program needn't handle non-finite values.
Results may differ from the reference program's by a relative error of at most 0.001.
Values may be sent and summed in bfloat16 or wider, within the bound.
A program may use at most 64 MiB of HBM per device.

```python
import jax
import jax.numpy as jnp
from jax import lax

D = 256
K = 65536
MASKED_DEV = 192
ITERS = 3
PATCH_DEV = 384
MASKED = 1536
PATCHES = 3072


def common_directions(key):
    return jax.random.normal(jax.random.fold_in(key, 7), (16, D), jnp.float32)


def draw_features(key, part):
    directions = common_directions(key)
    own_key = jax.random.fold_in(key, 41)
    first, second, third, fourth = jax.random.split(own_key, 4)
    groups = PATCHES // PATCH_DEV
    shifts = jax.random.normal(second, (groups, D), jnp.float32)
    amount = jax.random.uniform(third, (groups, 1), jnp.float32, 0.2, 1.0)
    picked = jax.random.randint(fourth, (groups,), 0, 16)
    aligned = 0.7 * jnp.take(directions, picked, axis=0)
    base = jax.random.normal(first, (PATCHES, D), jnp.float32)
    offset = jnp.repeat(shifts * amount + aligned, PATCH_DEV, axis=0)
    return jnp.clip(base + offset, -12.0, 12.0).astype(jnp.bfloat16)


def draw_prototypes(key, part):
    directions = common_directions(key)
    own_key = jax.random.fold_in(key, 43)
    block_ids = jnp.arange(K, dtype=jnp.int32) * 16 // K
    aligned = 0.6 * jnp.take(directions, block_ids, axis=0)
    base = jax.random.normal(own_key, (K, D), jnp.float32)
    return jnp.clip(base + aligned, -8.0, 8.0).astype(jnp.bfloat16)


def touch_ends(values, stream_key, smallest, largest):
    index_at = [jax.random.randint(jax.random.fold_in(stream_key, axis), (), 0, length) for axis, length in enumerate(values.shape)]
    widest = values.shape.index(max(values.shape))
    neighbour = index_at[:widest] + [(index_at[widest] + 1) % values.shape[widest]] + index_at[widest + 1:]
    return values.at[tuple(index_at)].set(smallest).at[tuple(neighbour)].set(largest)


def setup_inputs(seed: int = 0) -> dict:
    seeds = jax.random.split(jax.random.key(seed), 4)
    return {
        "features": draw_features(jax.random.fold_in(seeds[3], 71), 0),
        "prototypes": draw_prototypes(jax.random.fold_in(seeds[3], 71), 0),
        "masked_index": touch_ends(jax.random.randint(seeds[2], (MASKED,), 0, PATCH_DEV), jax.random.fold_in(seeds[2], 1), 0, PATCH_DEV - 1).astype(jnp.int32),
    }


TEMP = 0.07
EPS = 1e-06

def reference(features, prototypes, masked_index):
    owner = jnp.arange(MASKED, dtype=jnp.int32) // MASKED_DEV
    rowids = (owner * PATCH_DEV + masked_index).astype(jnp.int32)
    selected = jnp.take(features, rowids, axis=0)
    feat_scale = lax.rsqrt(lax.optimization_barrier(jnp.sum(jnp.square(selected.astype(jnp.float32)), axis=1)) + EPS)
    proto_scale = lax.rsqrt(lax.optimization_barrier(jnp.sum(jnp.square(prototypes.astype(jnp.float32)), axis=1)) + EPS)
    blocks = MASKED // MASKED_DEV
    protos_t = prototypes.T

    def weights_of(index):
        start = (index * MASKED_DEV).astype(jnp.int32)
        part = lax.dynamic_slice_in_dim(selected, start, MASKED_DEV, 0)
        scale = lax.dynamic_slice_in_dim(feat_scale, start, MASKED_DEV, 0)
        raw = jnp.dot(part, protos_t, preferred_element_type=jnp.float32)
        return jnp.exp(raw * scale[:, None] * proto_scale[None, :] / TEMP)

    def first_pass(total, index):
        return (total + lax.optimization_barrier(jnp.sum(weights_of(index), axis=0)), None)
    indices = jnp.arange(blocks, dtype=jnp.int32)
    col_mass, unused = lax.scan(first_pass, jnp.zeros((K,), jnp.float32), indices)
    for step in range(ITERS):
        col_scale = 1.0 / (K * col_mass)
        if step + 1 < ITERS:

            def middle(total, index):
                block = weights_of(index)
                row_mass = jnp.dot(block, col_scale, precision=lax.Precision.HIGHEST)
                row_scale = 1.0 / (MASKED * row_mass)
                return (total + jnp.dot(row_scale, block, precision=lax.Precision.HIGHEST), None)
            col_mass, unused = lax.scan(middle, jnp.zeros((K,), jnp.float32), indices)
        else:

            def final(carry, index):
                block = weights_of(index)
                row_mass = jnp.dot(block, col_scale, precision=lax.Precision.HIGHEST)
                row_scale = 1.0 / (MASKED * row_mass)
                result = float(K) * float(MASKED) * row_scale[:, None] * block * col_scale[None, :]
                return (carry, result.astype(jnp.bfloat16))
            unused, outputs = lax.scan(final, jnp.zeros((), jnp.float32), indices)
    return outputs.reshape(MASKED, K)
```

```python
import functools

import jax
import jax.numpy as jnp
from jax import lax
from jax.experimental import pallas as pl
from jax.experimental.pallas import tpu as pltpu
from jax.sharding import PartitionSpec as P

ITERS = 3


TEMP = 0.07
EPS = 1e-06
UP, DOWN, ACROSS = 0, 1, 2
LEAD = 2


def kernel(
    n_rows, n_protos, masked, protos_all,
    feat_ref, proto_ref, index_ref, weights_ref, rs_ref, cs_ref,
    feat_full, full, chosen, feat_scale, weights, acc, parts, masses, row_out, row_in,
    feat_send, feat_recv, own_sem, send, recv, out_sem,
    mass_send, mass_recv, scale_send, scale_recv, row_send, row_recv,
):
    r, p = lax.axis_index("rows"), lax.axis_index("protos")
    z, y = r // 2, lax.rem(r, 2)
    nz = n_rows // 2
    other = 1 - y
    dim, total = proto_ref.shape
    width = total // n_rows
    rows = index_ref.shape[0]
    fdim = feat_ref.shape[0]
    tile = min(512, width)
    tiles = width // tile
    mesh_id = pl.DeviceIdType.MESH

    barrier = pltpu.get_barrier_semaphore()
    for step in range(1, n_rows):
        pl.semaphore_signal(
            barrier, inc=1, device_id={"rows": lax.rem(r + step, n_rows)}, device_id_type=mesh_id
        )
    for step in range(1, n_protos):
        pl.semaphore_signal(
            barrier, inc=1, device_id={"protos": lax.rem(p + step, n_protos)}, device_id_type=mesh_id
        )
    pl.semaphore_wait(barrier, n_rows + n_protos - 2)

    def where(src, c):
        return (
            pl.ds(pl.multiple_of(src * dim, dim), dim),
            pl.ds(pl.multiple_of(c * width, width), width),
        )

    def block_copy(way, src, c, own=False):
        spot = where(src, c)
        target = {UP: r + 2, DOWN: r - 2, ACROSS: z * 2 + other}[way]
        return pltpu.make_async_remote_copy(
            src_ref=proto_ref.at[:, spot[1]] if own else full.at[spot],
            dst_ref=full.at[spot],
            send_sem=send.at[way, src, c],
            recv_sem=recv.at[src, c],
            device_id={"rows": target},
            device_id_type=mesh_id,
        )

    def own_copy(c):
        return pltpu.make_async_copy(
            proto_ref.at[:, where(r, c)[1]], full.at[where(r, c)], own_sem.at[c]
        )

    def send_own(c):
        @pl.when(z < nz - 1)
        def _():
            block_copy(UP, r, c, True).start()

        @pl.when(z > 0)
        def _():
            block_copy(DOWN, r, c, True).start()

        block_copy(ACROSS, r, c, True).start()
        own_copy(c).start()

    def feat_copy(step):
        block = pl.ds(pl.multiple_of(p * fdim, fdim), fdim)
        return pltpu.make_async_remote_copy(
            src_ref=feat_ref,
            dst_ref=feat_full.at[block],
            send_sem=feat_send.at[step],
            recv_sem=feat_recv.at[step],
            device_id={"protos": lax.rem(p + step, n_protos)},
            device_id_type=mesh_id,
        )

    for step in range(1, n_protos):
        feat_copy(step).start()
    for c in range(LEAD):
        send_own(c)
    feat_full[pl.ds(pl.multiple_of(p * fdim, fdim), fdim), :] = feat_ref[...]
    for step in range(1, n_protos):
        feat_copy(step).wait()
    onehot = lax.broadcasted_iota(jnp.int32, (rows, feat_ref.shape[1]), 1) == index_ref[...]
    picked = lax.dot_general(
        onehot.astype(jnp.float32).astype(jnp.bfloat16),
        feat_full[...],
        (((1,), (1,)), ((), ())),
        preferred_element_type=jnp.float32,
    )
    chosen[...] = picked.astype(jnp.bfloat16)
    scale = lax.rsqrt(jnp.sum(picked * picked, axis=1, keepdims=True) + EPS)
    feat_scale[...] = jnp.broadcast_to(scale * (1.0 / TEMP), feat_scale.shape)
    acc[...] = jnp.zeros_like(acc)

    def mass_copy(it, c, sender):
        return pltpu.make_async_remote_copy(
            src_ref=parts.at[it, c],
            dst_ref=masses.at[it, sender],
            send_sem=mass_send.at[it, c],
            recv_sem=mass_recv.at[it, sender],
            device_id={"rows": c},
            device_id_type=mesh_id,
        )

    def give_mass(it, c):
        @pl.when(c == r)
        def _():
            masses[it, c] = parts[it, c]

        @pl.when(c != r)
        def _():
            mass_copy(it, c, r).start()

    def out_copy(c):
        columns = where(r, c)[1]
        return pltpu.make_async_copy(
            weights.at[:, columns], weights_ref.at[:, columns], out_sem.at[c]
        )

    def make_weights(c):
        for t in range(tiles):
            columns = pl.ds(pl.multiple_of(c * width + t * tile, tile), tile)
            block = full[:, columns]
            wide = block.astype(jnp.float32)
            proto_scale = lax.rsqrt(jnp.sum(wide * wide, axis=0, keepdims=True) + EPS)
            raw = jnp.dot(chosen[...], block, preferred_element_type=jnp.float32)
            value = jnp.exp(raw * feat_scale[:, :1] * proto_scale)
            weights[:, columns] = value
            parts[0, c, :, t * tile:(t + 1) * tile] = jnp.sum(value, axis=0, keepdims=True)

    middle = n_rows // 2

    def line(c, d):
        for way, ahead, more, there in (
            (DOWN, z + d, z > 0, z + d < nz),
            (UP, z - d, z < nz - 1, z - d >= 0),
        ):
            src = ahead * 2 + y

            @pl.when(there)
            def _():
                block_copy(ACROSS, src, c).wait_recv()

                @pl.when(more)
                def _():
                    block_copy(way, src, c).start()

                @pl.when(c != middle)
                def _():
                    block_copy(ACROSS, src, c).start()

    def far_line(c, d):
        for way, ahead, more, there in (
            (DOWN, z + d, z > 0, z + d < nz),
            (UP, z - d, z < nz - 1, z - d >= 0),
        ):
            src = ahead * 2 + other

            @pl.when(there)
            def _():
                block_copy(ACROSS, src, c).wait_recv()

                @pl.when(jnp.logical_and(more, c == middle))
                def _():
                    block_copy(way, src, c).start()

    def beside(c):
        src = z * 2 + other
        block_copy(ACROSS, src, c).wait_recv()

        @pl.when(jnp.logical_and(z < nz - 1, c == middle))
        def _():
            block_copy(UP, src, c).start()

        @pl.when(jnp.logical_and(z > 0, c == middle))
        def _():
            block_copy(DOWN, src, c).start()

    def step_of(i, carry):
        @pl.when(i + LEAD < n_rows)
        def _():
            send_own(i + LEAD)

        @pl.when(i < n_rows)
        def _():
            beside(i)

        for d in range(1, nz):
            c = i - (d - 1)

            @pl.when(jnp.logical_and(c >= 0, c < n_rows))
            def _():
                line(c, d)

        last = i - (nz - 1)

        @pl.when(last >= 0)
        def _():
            for d in range(1, nz):
                far_line(last, d)
            own_copy(last).wait()
            make_weights(last)
            out_copy(last).start()
            give_mass(0, last)

        return carry

    lax.fori_loop(0, n_rows + nz - 1, step_of, 0)

    def scale_copy(it, c, step):
        return pltpu.make_async_remote_copy(
            src_ref=cs_ref.at[it, c],
            dst_ref=cs_ref.at[it, c],
            send_sem=scale_send.at[it, step],
            recv_sem=scale_recv.at[it, c],
            device_id={"rows": lax.rem(r + step, n_rows)},
            device_id_type=mesh_id,
        )

    def row_copy(it, step):
        return pltpu.make_async_remote_copy(
            src_ref=row_out.at[it],
            dst_ref=row_in.at[it, step],
            send_sem=row_send.at[it, step],
            recv_sem=row_recv.at[it, step],
            device_id={"protos": lax.rem(p + step, n_protos)},
            device_id_type=mesh_id,
        )

    for it in range(ITERS):
        if it > 0:
            row_scale = rs_ref[:rows, :1]

            def col_pass(j, carry):
                c = lax.rem(r + 1 + j, n_rows)
                for t in range(tiles):
                    columns = pl.ds(pl.multiple_of(c * width + t * tile, tile), tile)
                    value = jnp.sum(weights[:, columns] * rs_ref[:rows, :1], axis=0, keepdims=True)
                    parts[it, c, :, t * tile:(t + 1) * tile] = value
                give_mass(it, c)
                return carry

            lax.fori_loop(0, n_rows, col_pass, 0)
        for step in range(1, n_rows):
            mass_copy(it, r, lax.rem(r + step, n_rows)).wait_recv()
        cs_ref[it, r] = 1.0 / (protos_all * jnp.sum(masses[it], axis=0))
        for step in range(1, n_rows):
            scale_copy(it, r, step).start()

        def row_pass(j, total):
            c = lax.rem(r + j, n_rows)

            @pl.when(j > 0)
            def _():
                scale_copy(it, c, 1).wait_recv()

            for t in range(width // 128):
                columns = pl.ds(pl.multiple_of(c * width + t * 128, 128), 128)
                total = total + weights[:, columns] * cs_ref[it, c, :, t * 128:(t + 1) * 128]
            return total

        summed = lax.fori_loop(0, n_rows, row_pass, jnp.zeros((rows, 128), jnp.float32))
        acc[:rows, :] = summed
        row_out[it] = jnp.sum(acc[...].T, axis=0, keepdims=True)
        for step in range(1, n_protos):
            row_copy(it, step).start()
        mass = row_out[it]
        for step in range(1, n_protos):
            row_copy(it, step).wait_recv()
            mass = mass + row_in[it, step]
        turned = jnp.broadcast_to(1.0 / (masked * mass), (128, acc.shape[0])).T
        rs_ref[...] = turned

    for it in range(ITERS):
        for step in range(1, n_rows):
            mass_copy(it, lax.rem(r + step, n_rows), r).wait_send()
            scale_copy(it, r, step).wait_send()
        for step in range(1, n_protos):
            row_copy(it, step).wait_send()

    def drain(c, carry):
        out_copy(c).wait()
        for src_z in range(nz):
            for src_y in range(2):
                src = src_z * 2 + src_y
                on_line = src_y == y
                beside_me = jnp.logical_and(src_y != y, src_z == z)
                moved = jnp.logical_or(on_line, c == middle)

                @pl.when(jnp.logical_and(moved, jnp.logical_and(src_z <= z, z < nz - 1)))
                def _():
                    block_copy(UP, src, c).wait_send()

                @pl.when(jnp.logical_and(moved, jnp.logical_and(src_z >= z, z > 0)))
                def _():
                    block_copy(DOWN, src, c).wait_send()

                @pl.when(jnp.logical_and(on_line, jnp.logical_or(src_z == z, c != middle)))
                def _():
                    block_copy(ACROSS, src, c).wait_send()

        return carry

    lax.fori_loop(0, n_rows, drain, 0)


def with_kernel(n_rows, n_protos, features, prototypes, masked_index):
    rows = masked_index.shape[0]
    dim, total = prototypes.shape[1], prototypes.shape[0]
    fdim, patches = features.shape[1], features.shape[0]
    width = total // n_rows
    padded = -(-rows // 128) * 128
    masked = float(rows * n_rows)
    protos_all = float(total * n_protos)
    f32, bf16, dma = jnp.float32, jnp.bfloat16, pltpu.SemaphoreType.DMA
    vmem = pl.BlockSpec(memory_space=pltpu.VMEM)
    anywhere = pl.BlockSpec(memory_space=pl.ANY)
    weights, rs, cs = pl.pallas_call(
        functools.partial(kernel, n_rows, n_protos, masked, protos_all),
        out_shape=(
            jax.ShapeDtypeStruct((rows, total), f32),
            jax.ShapeDtypeStruct((padded, 128), f32),
            jax.ShapeDtypeStruct((ITERS, n_rows, 1, width), f32),
        ),
        in_specs=[vmem, anywhere, vmem],
        out_specs=(anywhere, vmem, vmem),
        scratch_shapes=[
            pltpu.VMEM((fdim * n_protos, patches), bf16),
            pltpu.VMEM((dim * n_rows, total), bf16),
            pltpu.VMEM((rows, fdim * n_protos), bf16),
            pltpu.VMEM((rows, 128), f32),
            pltpu.VMEM((rows, total), f32),
            pltpu.VMEM((padded, 128), f32),
            pltpu.VMEM((ITERS, n_rows, 1, width), f32),
            pltpu.VMEM((ITERS, n_rows, 1, width), f32),
            pltpu.VMEM((ITERS, 1, padded), f32),
            pltpu.VMEM((ITERS, n_protos, 1, padded), f32),
            dma((n_protos,)),
            dma((n_protos,)),
            dma((n_rows,)),
            dma((3, n_rows, n_rows)),
            dma((n_rows, n_rows)),
            dma((n_rows,)),
            dma((ITERS, n_rows)),
            dma((ITERS, n_rows)),
            dma((ITERS, n_rows)),
            dma((ITERS, n_rows)),
            dma((ITERS, n_protos)),
            dma((ITERS, n_protos)),
        ],
        compiler_params=pltpu.CompilerParams(
            collective_id=0, has_side_effects=True, vmem_limit_bytes=48 * 1024 * 1024
        ),
    )(features.T, prototypes.T, masked_index[:, None])
    row_scale = (protos_all * masked) * rs[:rows, :1]
    return (row_scale * weights * cs[ITERS - 1].reshape(1, total)).astype(jnp.bfloat16)


def with_collectives(features, prototypes, masked_index):
    total_protos = float(prototypes.shape[0] * lax.axis_size("protos"))
    chosen = jnp.take(features, masked_index, axis=0)
    patches = lax.all_gather(chosen, "protos", axis=1, tiled=True)
    feat_scale = lax.rsqrt(jnp.sum(jnp.square(patches.astype(jnp.float32)), axis=1) + EPS)
    full = lax.all_gather(prototypes, "rows", axis=1, tiled=True)
    proto_sq = jnp.sum(jnp.square(full.astype(jnp.float32)), axis=1)
    raw = lax.dot_general(
        patches, full, (((1,), (1,)), ((), ())), preferred_element_type=jnp.float32
    )
    proto_scale = lax.rsqrt(proto_sq + EPS)
    weights = jnp.exp(raw * feat_scale[:, None] * proto_scale[None, :] / TEMP)
    total_rows = masked_index.shape[0] * lax.axis_size("rows")
    row_scale = jnp.ones((patches.shape[0],), jnp.float32)
    for step in range(ITERS):
        col_part = jnp.dot(row_scale, weights, precision=lax.Precision.HIGHEST)
        col_scale = 1.0 / (total_protos * lax.psum(col_part, "rows"))
        row_part = jnp.dot(weights, col_scale, precision=lax.Precision.HIGHEST)
        row_scale = 1.0 / (total_rows * lax.psum(row_part, "protos"))
    factor = total_protos * float(total_rows)
    return (factor * row_scale[:, None] * weights * col_scale[None, :]).astype(jnp.bfloat16)


def solution(mesh):
    n_rows, n_protos = mesh.shape["rows"], mesh.shape["protos"]
    in_specs = (P("rows", "protos"), P("protos", "rows"), P("rows"))
    out_specs = P("rows", "protos")

    def on_device(features, prototypes, masked_index):
        fits = (
            n_rows % 2 == 0
            and n_rows <= 8
            and prototypes.shape[1] % 16 == 0
            and features.shape[1] % 16 == 0
            and prototypes.shape[0] % (n_rows * 128) == 0
        )
        if fits:
            return with_kernel(n_rows, n_protos, features, prototypes, masked_index)
        return with_collectives(features, prototypes, masked_index)

    return jax.shard_map(
        on_device, mesh=mesh, in_specs=in_specs, out_specs=out_specs, check_vma=False
    )
```

```python
import functools

import jax
import jax.numpy as jnp
from jax import lax
from jax.experimental import pallas as pl
from jax.experimental.pallas import tpu as pltpu
from jax.sharding import PartitionSpec as P

ITERS = 3


TEMP = 0.07
EPS = 1e-06
UP, DOWN, ACROSS = 0, 1, 2
LEAD = 2
SPLIT = 1


def kernel(
    n_rows, n_protos, masked, protos_all,
    feat_ref, proto_ref, index_ref, weights, rs_ref, cs_ref,
    feat_full, index, onehot, full, chosen, feat_scale, acc, parts, masses, row_out, row_in,
    feat_send, feat_recv, in_sem, own_sem, send, recv,
    mass_send, mass_recv, scale_send, scale_recv, row_send, row_recv,
):
    r, p = lax.axis_index("rows"), lax.axis_index("protos")
    z, y = r // 2, lax.rem(r, 2)
    nz = n_rows // 2
    other = 1 - y
    dim, total = proto_ref.shape
    width = total // n_rows
    chunks = n_rows * SPLIT
    span = total // chunks
    rows = weights.shape[0]
    fdim = feat_ref.shape[0]
    tile = min(512, span)
    tiles = width // tile
    mesh_id = pl.DeviceIdType.MESH

    barrier = pltpu.get_barrier_semaphore()
    for step in range(1, n_rows):
        pl.semaphore_signal(
            barrier, inc=1, device_id={"rows": lax.rem(r + step, n_rows)}, device_id_type=mesh_id
        )
    for step in range(1, n_protos):
        pl.semaphore_signal(
            barrier, inc=1, device_id={"protos": lax.rem(p + step, n_protos)}, device_id_type=mesh_id
        )
    pl.semaphore_wait(barrier, n_rows + n_protos - 2)

    def where(src, c):
        return full.at[c, pl.ds(pl.multiple_of(src * dim, dim), dim)]

    def given(c):
        return proto_ref.at[:, pl.ds(pl.multiple_of(c * span, span), span)]

    def block_copy(way, src, c, own=False):
        target = {UP: r + 2, DOWN: r - 2, ACROSS: z * 2 + other}[way]
        return pltpu.make_async_remote_copy(
            src_ref=given(c) if own else where(src, c),
            dst_ref=where(src, c),
            send_sem=send.at[way, src, c],
            recv_sem=recv.at[src, c],
            device_id={"rows": target},
            device_id_type=mesh_id,
        )

    def own_copy(c):
        return pltpu.make_async_copy(given(c), where(r, c), own_sem.at[c])

    def send_own(c):
        @pl.when(z < nz - 1)
        def _():
            block_copy(UP, r, c, True).start()

        @pl.when(z > 0)
        def _():
            block_copy(DOWN, r, c, True).start()

        block_copy(ACROSS, r, c, True).start()
        own_copy(c).start()

    def feat_copy(step):
        block = pl.ds(pl.multiple_of(p * fdim, fdim), fdim)
        return pltpu.make_async_remote_copy(
            src_ref=feat_ref,
            dst_ref=feat_full.at[block],
            send_sem=feat_send.at[step],
            recv_sem=feat_recv.at[step],
            device_id={"protos": lax.rem(p + step, n_protos)},
            device_id_type=mesh_id,
        )

    index_in = pltpu.make_async_copy(index_ref, index, in_sem.at[0])
    feat_in = pltpu.make_async_copy(
        feat_ref, feat_full.at[pl.ds(pl.multiple_of(p * fdim, fdim), fdim)], in_sem.at[1]
    )
    for step in range(1, n_protos):
        feat_copy(step).start()
    for c in range(LEAD):
        send_own(c)
    index_in.start()
    feat_in.start()
    onehot[...] = jnp.zeros_like(onehot)
    index_in.wait()
    hits = lax.broadcasted_iota(jnp.int32, (onehot.shape[0], rows), 0) == index[...]
    onehot[:, :rows] = hits.astype(jnp.float32).astype(jnp.bfloat16)
    feat_in.wait()
    for step in range(1, n_protos):
        feat_copy(step).wait()
    picked = jnp.dot(feat_full[...], onehot[...], preferred_element_type=jnp.float32)
    picked = picked.T[:rows]
    chosen[...] = picked.astype(jnp.bfloat16)
    scale = lax.rsqrt(jnp.sum(picked * picked, axis=1, keepdims=True) + EPS)
    feat_scale[...] = jnp.broadcast_to(scale * (1.0 / TEMP), feat_scale.shape)
    acc[...] = jnp.zeros_like(acc)

    def mass_copy(it, c, sender):
        return pltpu.make_async_remote_copy(
            src_ref=parts.at[it, c],
            dst_ref=masses.at[it, sender],
            send_sem=mass_send.at[it, c],
            recv_sem=mass_recv.at[it, sender],
            device_id={"rows": c},
            device_id_type=mesh_id,
        )

    def give_mass(it, c):
        @pl.when(c == r)
        def _():
            masses[it, c] = parts[it, c]

        @pl.when(c != r)
        def _():
            mass_copy(it, c, r).start()

    def make_weights(c):
        for t in range(span // tile):
            columns = pl.ds(pl.multiple_of(c * span + t * tile, tile), tile)
            within = pl.ds(pl.multiple_of(lax.rem(c, SPLIT) * span + t * tile, tile), tile)
            block = full[c, :, t * tile:(t + 1) * tile]
            wide = block.astype(jnp.float32)
            proto_scale = lax.rsqrt(jnp.sum(wide * wide, axis=0, keepdims=True) + EPS)
            raw = jnp.dot(chosen[...], block, preferred_element_type=jnp.float32)
            value = jnp.exp(raw * feat_scale[:, :1] * proto_scale)
            weights[:, columns] = value
            parts[0, c // SPLIT, :, within] = jnp.sum(value, axis=0, keepdims=True)

    def early(c):
        return c == 4

    def line(c, d):
        for way, ahead, more, there in (
            (DOWN, z + d, z > 0, z + d < nz),
            (UP, z - d, z < nz - 1, z - d >= 0),
        ):
            src = ahead * 2 + y

            @pl.when(there)
            def _():
                block_copy(ACROSS, src, c).wait_recv()

                @pl.when(more)
                def _():
                    block_copy(way, src, c).start()

                @pl.when(jnp.logical_not(early(c)))
                def _():
                    block_copy(ACROSS, src, c).start()

    def far_line(c, d):
        for way, ahead, more, there in (
            (DOWN, z + d, z > 0, z + d < nz),
            (UP, z - d, z < nz - 1, z - d >= 0),
        ):
            src = ahead * 2 + other

            @pl.when(there)
            def _():
                block_copy(ACROSS, src, c).wait_recv()

                @pl.when(jnp.logical_and(more, early(c)))
                def _():
                    block_copy(way, src, c).start()

    def beside(c):
        src = z * 2 + other
        block_copy(ACROSS, src, c).wait_recv()

        @pl.when(jnp.logical_and(z < nz - 1, early(c)))
        def _():
            block_copy(UP, src, c).start()

        @pl.when(jnp.logical_and(z > 0, early(c)))
        def _():
            block_copy(DOWN, src, c).start()

    def step_of(i, carry):
        @pl.when(i + LEAD < chunks)
        def _():
            send_own(i + LEAD)

        @pl.when(i < chunks)
        def _():
            beside(i)

        for d in range(1, nz):
            c = i - (d - 1)

            @pl.when(jnp.logical_and(c >= 0, c < chunks))
            def _():
                line(c, d)

        for d in range(1, nz):
            c = i - d

            @pl.when(jnp.logical_and(jnp.logical_and(c >= 0, c < chunks), early(c)))
            def _():
                far_line(c, d)

        last = i - (nz - 1)

        @pl.when(jnp.logical_and(last >= 0, jnp.logical_not(early(last))))
        def _():
            for d in range(1, nz):
                far_line(last, d)

        @pl.when(last >= 0)
        def _():
            own_copy(last).wait()
            make_weights(last)

            @pl.when(lax.rem(last, SPLIT) == SPLIT - 1)
            def _():
                give_mass(0, last // SPLIT)

        return carry

    lax.fori_loop(0, chunks + nz - 1, step_of, 0)

    def scale_copy(it, c, step):
        return pltpu.make_async_remote_copy(
            src_ref=cs_ref.at[it, c],
            dst_ref=cs_ref.at[it, c],
            send_sem=scale_send.at[it, step],
            recv_sem=scale_recv.at[it, c],
            device_id={"rows": lax.rem(r + step, n_rows)},
            device_id_type=mesh_id,
        )

    def row_copy(it, step):
        return pltpu.make_async_remote_copy(
            src_ref=row_out.at[it],
            dst_ref=row_in.at[it, step],
            send_sem=row_send.at[it, step],
            recv_sem=row_recv.at[it, step],
            device_id={"protos": lax.rem(p + step, n_protos)},
            device_id_type=mesh_id,
        )

    for it in range(ITERS):
        if it > 0:
            row_scale = rs_ref[:rows, :1]

            def col_pass(j, carry):
                c = lax.rem(r + 1 + j, n_rows)
                for t in range(tiles):
                    columns = pl.ds(pl.multiple_of(c * width + t * tile, tile), tile)
                    value = jnp.sum(weights[:, columns] * rs_ref[:rows, :1], axis=0, keepdims=True)
                    parts[it, c, :, t * tile:(t + 1) * tile] = value
                give_mass(it, c)
                return carry

            lax.fori_loop(0, n_rows, col_pass, 0)
        for step in range(1, n_rows):
            mass_copy(it, r, lax.rem(r + step, n_rows)).wait_recv()
        cs_ref[it, r] = 1.0 / (protos_all * jnp.sum(masses[it], axis=0))
        for step in range(1, n_rows):
            scale_copy(it, r, step).start()

        def row_pass(j, total):
            c = lax.rem(r + j, n_rows)

            @pl.when(j > 0)
            def _():
                scale_copy(it, c, 1).wait_recv()

            for t in range(width // 128):
                columns = pl.ds(pl.multiple_of(c * width + t * 128, 128), 128)
                total = total + weights[:, columns] * cs_ref[it, c, :, t * 128:(t + 1) * 128]
            return total

        summed = lax.fori_loop(0, n_rows, row_pass, jnp.zeros((rows, 128), jnp.float32))
        acc[:rows, :] = summed
        row_out[it] = jnp.sum(acc[...].T, axis=0, keepdims=True)
        for step in range(1, n_protos):
            row_copy(it, step).start()
        mass = row_out[it]
        for step in range(1, n_protos):
            row_copy(it, step).wait_recv()
            mass = mass + row_in[it, step]
        turned = jnp.broadcast_to(1.0 / (masked * mass), (128, acc.shape[0])).T
        rs_ref[...] = turned

    for it in range(ITERS):
        for step in range(1, n_rows):
            mass_copy(it, lax.rem(r + step, n_rows), r).wait_send()
            scale_copy(it, r, step).wait_send()
        for step in range(1, n_protos):
            row_copy(it, step).wait_send()

    def drain(c, carry):
        for src_z in range(nz):
            for src_y in range(2):
                src = src_z * 2 + src_y
                on_line = src_y == y
                beside_me = jnp.logical_and(src_y != y, src_z == z)
                moved = jnp.logical_or(on_line, early(c))

                @pl.when(jnp.logical_and(moved, jnp.logical_and(src_z <= z, z < nz - 1)))
                def _():
                    block_copy(UP, src, c).wait_send()

                @pl.when(jnp.logical_and(moved, jnp.logical_and(src_z >= z, z > 0)))
                def _():
                    block_copy(DOWN, src, c).wait_send()

                @pl.when(jnp.logical_and(on_line, jnp.logical_or(src_z == z, jnp.logical_not(early(c)))))
                def _():
                    block_copy(ACROSS, src, c).wait_send()

        return carry

    lax.fori_loop(0, chunks, drain, 0)


def finish(factor, weights, rs_ref, cs_ref, out_ref, buffer, out_sem):
    rows, total = weights.shape
    count, width = cs_ref.shape[0], cs_ref.shape[2]
    slots = buffer.shape[0]

    def out_copy(c):
        columns = pl.ds(pl.multiple_of(c * width, width), width)
        slot = lax.rem(c, slots)
        return pltpu.make_async_copy(buffer.at[slot], out_ref.at[:, columns], out_sem.at[slot])

    def block(c, carry):
        @pl.when(c >= slots)
        def _():
            out_copy(c - slots).wait()

        for t in range(width // 128):
            columns = pl.ds(pl.multiple_of(c * width + t * 128, 128), 128)
            col_scale = cs_ref[c, :, t * 128:(t + 1) * 128]
            value = (factor * rs_ref[:rows, :]) * weights[:, columns] * col_scale
            buffer[lax.rem(c, slots), :, t * 128:(t + 1) * 128] = value.astype(jnp.bfloat16)
        out_copy(c).start()
        return carry

    lax.fori_loop(0, count, block, 0)
    for c in range(max(0, count - slots), count):
        out_copy(c).wait()


def with_kernel(n_rows, n_protos, features, prototypes, masked_index):
    rows = masked_index.shape[0]
    dim, total = prototypes.shape[1], prototypes.shape[0]
    fdim, patches = features.shape[1], features.shape[0]
    width = total // n_rows
    padded = -(-rows // 128) * 128
    masked = float(rows * n_rows)
    protos_all = float(total * n_protos)
    f32, bf16, dma = jnp.float32, jnp.bfloat16, pltpu.SemaphoreType.DMA
    vmem = pl.BlockSpec(memory_space=pltpu.VMEM)
    anywhere = pl.BlockSpec(memory_space=pl.ANY)
    weights, rs, cs = pl.pallas_call(
        functools.partial(kernel, n_rows, n_protos, masked, protos_all),
        out_shape=(
            jax.ShapeDtypeStruct((rows, total), f32),
            jax.ShapeDtypeStruct((padded, 128), f32),
            jax.ShapeDtypeStruct((ITERS, n_rows, 1, width), f32),
        ),
        in_specs=[pl.BlockSpec(memory_space=pltpu.HBM)] * 3,
        out_specs=(vmem, vmem, vmem),
        scratch_shapes=[
            pltpu.VMEM((fdim * n_protos, patches), bf16),
            pltpu.VMEM((1, rows), jnp.int32),
            pltpu.VMEM((patches, padded), bf16),
            pltpu.VMEM((n_rows * SPLIT, dim * n_rows, width // SPLIT), bf16),
            pltpu.VMEM((rows, fdim * n_protos), bf16),
            pltpu.VMEM((rows, 128), f32),
            pltpu.VMEM((padded, 128), f32),
            pltpu.VMEM((ITERS, n_rows, 1, width), f32),
            pltpu.VMEM((ITERS, n_rows, 1, width), f32),
            pltpu.VMEM((ITERS, 1, padded), f32),
            pltpu.VMEM((ITERS, n_protos, 1, padded), f32),
            dma((n_protos,)),
            dma((n_protos,)),
            dma((2,)),
            dma((n_rows * SPLIT,)),
            dma((3, n_rows, n_rows * SPLIT)),
            dma((n_rows, n_rows * SPLIT)),
            dma((ITERS, n_rows)),
            dma((ITERS, n_rows)),
            dma((ITERS, n_rows)),
            dma((ITERS, n_rows)),
            dma((ITERS, n_protos)),
            dma((ITERS, n_protos)),
        ],
        compiler_params=pltpu.CompilerParams(
            collective_id=0, has_side_effects=True, vmem_limit_bytes=20 * 1024 * 1024
        ),
    )(features.T, prototypes.T, masked_index[None, :])
    return pl.pallas_call(
        functools.partial(finish, protos_all * masked),
        out_shape=jax.ShapeDtypeStruct((rows, total), bf16),
        in_specs=[vmem, vmem, vmem],
        out_specs=anywhere,
        scratch_shapes=[pltpu.VMEM((4, rows, width), bf16), dma((4,))],
        compiler_params=pltpu.CompilerParams(vmem_limit_bytes=20 * 1024 * 1024),
    )(weights, rs, cs[ITERS - 1])


def with_collectives(features, prototypes, masked_index):
    total_protos = float(prototypes.shape[0] * lax.axis_size("protos"))
    chosen = jnp.take(features, masked_index, axis=0)
    patches = lax.all_gather(chosen, "protos", axis=1, tiled=True)
    feat_scale = lax.rsqrt(jnp.sum(jnp.square(patches.astype(jnp.float32)), axis=1) + EPS)
    full = lax.all_gather(prototypes, "rows", axis=1, tiled=True)
    proto_sq = jnp.sum(jnp.square(full.astype(jnp.float32)), axis=1)
    raw = lax.dot_general(
        patches, full, (((1,), (1,)), ((), ())), preferred_element_type=jnp.float32
    )
    proto_scale = lax.rsqrt(proto_sq + EPS)
    weights = jnp.exp(raw * feat_scale[:, None] * proto_scale[None, :] / TEMP)
    total_rows = masked_index.shape[0] * lax.axis_size("rows")
    row_scale = jnp.ones((patches.shape[0],), jnp.float32)
    for step in range(ITERS):
        col_part = jnp.dot(row_scale, weights, precision=lax.Precision.HIGHEST)
        col_scale = 1.0 / (total_protos * lax.psum(col_part, "rows"))
        row_part = jnp.dot(weights, col_scale, precision=lax.Precision.HIGHEST)
        row_scale = 1.0 / (total_rows * lax.psum(row_part, "protos"))
    factor = total_protos * float(total_rows)
    return (factor * row_scale[:, None] * weights * col_scale[None, :]).astype(jnp.bfloat16)


def solution(mesh):
    n_rows, n_protos = mesh.shape["rows"], mesh.shape["protos"]
    in_specs = (P("rows", "protos"), P("protos", "rows"), P("rows"))
    out_specs = P("rows", "protos")

    def on_device(features, prototypes, masked_index):
        fits = (
            n_rows % 2 == 0
            and n_rows <= 8
            and prototypes.shape[1] % 16 == 0
            and features.shape[1] % 16 == 0
            and prototypes.shape[0] % (n_rows * SPLIT * 128) == 0
        )
        if fits:
            return with_kernel(n_rows, n_protos, features, prototypes, masked_index)
        return with_collectives(features, prototypes, masked_index)

    return jax.shard_map(
        on_device, mesh=mesh, in_specs=in_specs, out_specs=out_specs, check_vma=False
    )
```
